16 devices in a mesh: data: 4 (over z, y), tp: 4 (over x, core).
Axes of the slice: x: 2, y: 2, z: 2, core: 2. Of those that a mesh axis runs over, the one named last changes fastest.
Arguments:
- x_one: bfloat16 [1024, 49152], P('data', 'tp'), parts along dimension 0
- x_two: bfloat16 [1024, 49152], P('data', 'tp'), parts along dimension 0
- w_down: bfloat16 [49152, 12288], P('tp')
Outputs:
- output 1: bfloat16 [1024, 12288], P('data'), parts along dimension 0
- output 2: bfloat16 [1024, 12288], P('data'), parts along dimension 0
There are 4 independent parts. The reference program is written for one: setup_inputs(seed, part) draws one part's arguments, and reference() takes and returns one part's arrays. A program takes and returns all parts, laid end to end along the dimension named above; an argument that names none is the same for every part.
All inputs are finite; a program needn't handle non-finite values.
Results may differ from the reference program's by a relative error of at most 0.010606.
Values are sent between devices in bfloat16 or wider.
A program may use at most 1.25 GiB of HBM per device.

```python
import jax
import jax.numpy as jnp

F = 49152
H = 12288
MB = 256


def setup_inputs(seed: int = 0, part: int = 0) -> dict:
    base_key = jax.random.key(seed)
    part_key = jax.random.fold_in(base_key, part)
    x_one = jax.random.normal(jax.random.fold_in(part_key, 1), (MB, F), jnp.float32).astype(jnp.bfloat16)
    x_two = jax.random.normal(jax.random.fold_in(part_key, 2), (MB, F), jnp.float32).astype(jnp.bfloat16)
    w_down = (jax.random.normal(jax.random.fold_in(base_key, 3), (F, H), jnp.float32) * (F ** -0.5)).astype(jnp.bfloat16)
    return {"x_one": x_one, "x_two": x_two, "w_down": w_down}


def reference(x_one, x_two, w_down):
    y_one = jnp.dot(x_one, w_down, preferred_element_type=jnp.float32).astype(jnp.bfloat16)
    y_two = jnp.dot(x_two, w_down, preferred_element_type=jnp.float32).astype(jnp.bfloat16)
    return (y_one, y_two)
```

```python
import jax
import jax.numpy as jnp
from jax import lax
from jax.experimental import pallas as pl
from jax.experimental.pallas import tpu as pltpu
from jax.sharding import PartitionSpec as P

MESH = pl.DeviceIdType.MESH
BF16 = jnp.bfloat16
F32 = jnp.float32

COLS = 512
PIECES = 6


def mod(j, n):
    return j % n if isinstance(j, int) else lax.rem(j, n)


def kernel(x1, x2, w, y1, y2, X, W, Ps, R, own, A, B, Y,
           xsem, w0sem, wsem, p_send, p_recv, a_send, a_recv, y_loc, y_send, y_recv):
    mb, depth = x1.shape
    width = w.shape[1]
    half = mb // 2
    n = width // COLS
    kp = depth // PIECES

    me = lax.axis_index("tp")
    core = lax.rem(me, 2)
    sib = me + 1 - 2 * core
    peer = lax.rem(me + 2, 4)
    r_own = pl.multiple_of(core * half, half)
    r_oth = pl.multiple_of((1 - core) * half, half)

    def col(j):
        return pl.ds(j * COLS if isinstance(j, int) else pl.multiple_of(j * COLS, COLS), COLS)

    def x_copies(i):
        ks = pl.ds(i * kp if isinstance(i, int) else pl.multiple_of(i * kp, kp), kp)
        return [
            pltpu.make_async_copy(src.at[pl.ds(row, half), ks], X.at[pl.ds(g * half, half), ks], xsem.at[i, g])
            for g, (src, row) in enumerate(((x1, r_oth), (x2, r_oth), (x1, r_own), (x2, r_own)))
        ]

    def w0_copy(i):
        ks = pl.ds(i * kp if isinstance(i, int) else pl.multiple_of(i * kp, kp), kp)
        return pltpu.make_async_copy(w.at[ks, col(0)], W.at[0, ks], w0sem.at[i])

    def w_copies(j):
        s = mod(j, 3)
        kh = depth // 2
        return [
            pltpu.make_async_copy(w.at[pl.ds(i * kh, kh), col(j)], W.at[s, pl.ds(i * kh, kh)], wsem.at[s, i])
            for i in range(2)
        ]

    def p_copy(j):
        s = mod(j, 2)
        return pltpu.make_async_remote_copy(
            src_ref=Ps.at[s], dst_ref=R.at[s], send_sem=p_send.at[s], recv_sem=p_recv.at[s],
            device_id={"tp": sib}, device_id_type=MESH)

    def a_copy(j):
        s, t = mod(j, 4), mod(j, 5)
        return pltpu.make_async_remote_copy(
            src_ref=A.at[s], dst_ref=B.at[t], send_sem=a_send.at[s], recv_sem=a_recv.at[t],
            device_id={"tp": peer}, device_id_type=MESH)

    def y_copies(j):
        s, t = mod(j, 2), mod(j, 4)
        out = []
        for g, y in enumerate((y1, y2)):
            src = Y.at[s, pl.ds(g * half, half)]
            dst = y.at[pl.ds(r_own, half), col(j)]
            out.append(pltpu.make_async_copy(src, dst, y_loc.at[s, g]))
            out.append(pltpu.make_async_remote_copy(
                src_ref=src, dst_ref=dst, send_sem=y_send.at[s, g], recv_sem=y_recv.at[t, g],
                device_id={"tp": sib}, device_id_type=MESH))
        return out

    def start(copies):
        for c in copies:
            c.start()

    def wait(copies):
        for c in copies:
            c.wait()

    def pair_sum(j):
        A[mod(j, 4)] = (own[...] + R[mod(j, 2)]).astype(BF16)

    def total(j, a, b):
        Y[mod(j, 2)] = (A[a].astype(F32) + B[b].astype(F32)).astype(BF16)

    def mul_oth(j):
        Ps[mod(j, 2)] = jnp.dot(X[pl.ds(0, mb), :], W[mod(j, 3)], preferred_element_type=F32)

    def mul_own(j):
        own[...] = jnp.dot(X[pl.ds(mb, mb), :], W[mod(j, 3)], preferred_element_type=F32)

    for i in range(PIECES):
        start(x_copies(i))
        w0_copy(i).start()
    for j in (1, 2):
        start(w_copies(j))

    barrier = pltpu.get_barrier_semaphore()
    for other in (sib, peer):
        pl.semaphore_signal(barrier, inc=1, device_id={"tp": other}, device_id_type=MESH)
    pl.semaphore_wait(barrier, 2)

    Ps[0] = jnp.zeros((mb, COLS), F32)
    own[...] = jnp.zeros((mb, COLS), F32)

    def first(i, carry):
        w0_copy(i).wait()
        wait(x_copies(i))
        ks = pl.ds(pl.multiple_of(i * kp, kp), kp)
        d = jnp.dot(X[:, ks], W[0, ks, :], preferred_element_type=F32)
        Ps[0] += d[:mb]
        own[...] += d[mb:]
        return carry

    lax.fori_loop(0, PIECES, first, 0)
    p_copy(0).start()
    wait(w_copies(1))
    mul_oth(1)

    def bound(j, guard):
        wait(w_copies(j + 1))
        p_copy(j - 1).wait()
        pair_sum(j - 1)
        p_copy(j).start()
        start(w_copies(j + 2))
        guard(j >= 3, lambda: a_copy(j - 3).wait())
        guard(j >= 5, lambda: wait(y_copies(j - 5)))
        a_copy(j - 1).start()
        guard(j >= 4, lambda: start(y_copies(j - 4)))

    def step(j, carry):
        bound(j, lambda c, f: pl.when(c)(f))
        total(j + 1, mod(j + 1, 4), mod(j + 2, 5))
        mul_oth(j + 1)
        mul_own(j)
        return carry

    m = n - 3
    lax.fori_loop(1, m, step, 0)

    def tot(j):
        total(j, j % 4, j % 5)

    bound(m, lambda c, f: f())
    tot(m - 3)
    mul_own(m)

    p_copy(m).wait()
    pair_sum(m)
    a_copy(m - 2).wait()
    wait(y_copies(m - 4))
    a_copy(m).start()
    start(y_copies(m - 3))
    tot(m - 2)
    mul_oth(m + 1)

    p_copy(m + 1).start()
    start(y_copies(m - 2))
    wait(w_copies(m + 2))
    wait(y_copies(m - 3))
    mul_own(m + 1)

    p_copy(m + 1).wait()
    pair_sum(m + 1)
    a_copy(m - 1).wait()
    a_copy(m + 1).start()
    tot(m - 1)
    mul_oth(m + 2)

    wait(y_copies(m - 2))
    p_copy(m + 2).start()
    start(y_copies(m - 1))
    a_copy(m).wait()
    tot(m)
    mul_own(m + 2)

    p_copy(m + 2).wait()
    pair_sum(m + 2)
    wait(y_copies(m - 1))
    start(y_copies(m))
    a_copy(m + 2).start()
    a_copy(m + 1).wait()
    tot(m + 1)
    wait(y_copies(m))
    start(y_copies(m + 1))
    a_copy(m + 2).wait()
    tot(m + 2)
    start(y_copies(m + 2))
    wait(y_copies(m + 1))
    wait(y_copies(m + 2))


def solution(mesh):
    def per_device(x_one, x_two, w_down):
        mb, depth = x_one.shape
        width = w_down.shape[1]
        hbm = pl.BlockSpec(memory_space=pltpu.HBM)
        dma = pltpu.SemaphoreType.DMA
        return pl.pallas_call(
            kernel,
            out_shape=[jax.ShapeDtypeStruct((mb, width), BF16)] * 2,
            in_specs=[hbm] * 3,
            out_specs=[hbm] * 2,
            scratch_shapes=[
                pltpu.VMEM((2 * mb, depth), BF16),
                pltpu.VMEM((3, depth, COLS), BF16),
                pltpu.VMEM((2, mb, COLS), F32),
                pltpu.VMEM((2, mb, COLS), F32),
                pltpu.VMEM((mb, COLS), F32),
                pltpu.VMEM((4, mb, COLS), BF16),
                pltpu.VMEM((5, mb, COLS), BF16),
                pltpu.VMEM((2, mb, COLS), BF16),
                dma((PIECES, 4)), dma((PIECES,)), dma((3, 2)),
                dma((2,)), dma((2,)), dma((4,)), dma((5,)),
                dma((2, 2)), dma((2, 2)), dma((4, 2)),
            ],
            compiler_params=pltpu.CompilerParams(
                collective_id=0, has_side_effects=True, vmem_limit_bytes=60 * 1024 * 1024),
        )(x_one, x_two, w_down)

    return jax.shard_map(
        per_device,
        mesh=mesh,
        in_specs=(P("data", "tp"), P("data", "tp"), P("tp", None)),
        out_specs=(P("data", None), P("data", None)),
        check_vma=False,
    )
```

```python
import jax
import jax.numpy as jnp
from jax import lax
from jax.experimental import pallas as pl
from jax.experimental.pallas import tpu as pltpu
from jax.sharding import PartitionSpec as P

MESH = pl.DeviceIdType.MESH
BF16 = jnp.bfloat16
F32 = jnp.float32

COLS = 512
PIECES = 6


def mod(j, n):
    return j % n if isinstance(j, int) else lax.rem(j, n)


def kernel(x1, x2, w, y1, y2, X, W, Ps, R, own, A, B,
           xsem, w0sem, wsem, p_send, p_recv, a_send, a_recv, y_send, y_recv):
    mb, depth = x1.shape
    width = w.shape[1]
    half = mb // 2
    n = width // COLS
    kp = depth // PIECES

    me = lax.axis_index("tp")
    core = lax.rem(me, 2)
    sib = me + 1 - 2 * core
    peer = lax.rem(me + 2, 4)
    r_own = pl.multiple_of(core * half, half)
    r_oth = pl.multiple_of((1 - core) * half, half)

    def col(j):
        return pl.ds(j * COLS if isinstance(j, int) else pl.multiple_of(j * COLS, COLS), COLS)

    def x_copies(i):
        ks = pl.ds(i * kp if isinstance(i, int) else pl.multiple_of(i * kp, kp), kp)
        return [
            pltpu.make_async_copy(src.at[pl.ds(row, half), ks], X.at[pl.ds(g * half, half), ks], xsem.at[i, g])
            for g, (src, row) in enumerate(((x1, r_oth), (x2, r_oth), (x1, r_own), (x2, r_own)))
        ]

    def w0_copy(i):
        ks = pl.ds(i * kp if isinstance(i, int) else pl.multiple_of(i * kp, kp), kp)
        return pltpu.make_async_copy(w.at[ks, col(0)], W.at[0, ks], w0sem.at[i])

    def w_copies(j):
        s = mod(j, 2)
        kh = depth // 2
        return [
            pltpu.make_async_copy(w.at[pl.ds(i * kh, kh), col(j)], W.at[s, pl.ds(i * kh, kh)], wsem.at[s, i])
            for i in range(2)
        ]

    def p_copy(j):
        s = mod(j, 2)
        return pltpu.make_async_remote_copy(
            src_ref=Ps.at[s], dst_ref=R.at[s], send_sem=p_send.at[s], recv_sem=p_recv.at[s],
            device_id={"tp": sib}, device_id_type=MESH)

    def a_copy(j):
        s, t = mod(j, 4), mod(j, 8)
        return pltpu.make_async_remote_copy(
            src_ref=A.at[s], dst_ref=B.at[t], send_sem=a_send.at[s], recv_sem=a_recv.at[t],
            device_id={"tp": peer}, device_id_type=MESH)

    def y_copies(j):
        s, t = mod(j, 2), mod(j, 4)
        out = []
        for g, y in enumerate((y1, y2)):
            ref = y.at[pl.ds(r_own, half), col(j)]
            out.append(pltpu.make_async_remote_copy(
                src_ref=ref, dst_ref=ref, send_sem=y_send.at[s, g], recv_sem=y_recv.at[t, g],
                device_id={"tp": sib}, device_id_type=MESH))
        return out

    def start(copies):
        for c in copies:
            c.start()

    def wait(copies):
        for c in copies:
            c.wait()

    def pair_sum(j):
        A[mod(j, 4)] = (own[mod(j, 2)] + R[mod(j, 2)]).astype(BF16)

    def total(j, c=None):
        v = (A[mod(j, 4)].astype(F32) + B[mod(j, 8)].astype(F32)).astype(BF16)
        for g, y in enumerate((y1, y2)):
            y[pl.ds(r_own, half), col(j if c is None else c)] = v[g * half : (g + 1) * half]

    def mul(j):
        s = mod(j, 2)
        d = jnp.dot(X[...], W[s], preferred_element_type=F32)
        Ps[s] = d[:mb]
        own[s] = d[mb:]

    def mul_oth(j):
        Ps[j % 2] = jnp.dot(X[pl.ds(0, mb), :], W[j % 2], preferred_element_type=F32)

    def mul_own(j):
        own[j % 2] = jnp.dot(X[pl.ds(mb, mb), :], W[j % 2], preferred_element_type=F32)

    for i in range(PIECES):
        start(x_copies(i))
        w0_copy(i).start()
    start(w_copies(1))

    barrier = pltpu.get_barrier_semaphore()
    for other in (sib, peer):
        pl.semaphore_signal(barrier, inc=1, device_id={"tp": other}, device_id_type=MESH)
    pl.semaphore_wait(barrier, 2)

    Ps[0] = jnp.zeros((mb, COLS), F32)
    own[0] = jnp.zeros((mb, COLS), F32)

    def first(i, carry):
        w0_copy(i).wait()
        wait(x_copies(i))
        ks = pl.ds(pl.multiple_of(i * kp, kp), kp)
        d = jnp.dot(X[:, ks], W[0, ks, :], preferred_element_type=F32)
        Ps[0] += d[:mb]
        own[0] += d[mb:]
        return carry

    lax.fori_loop(0, PIECES, first, 0)

    def bound(j, guard):
        wait(w_copies(j))

        guard(j >= 2, lambda: p_copy(j - 2).wait())
        pair_sum(j - 2 if isinstance(j, int) else j + 2)
        p_copy(j - 1).start()
        start(w_copies(j + 1))
        guard(j >= 4, lambda: a_copy(j - 4).wait())
        guard(j >= 6, lambda: wait(y_copies(j - 6)))
        guard(j >= 2, lambda: a_copy(j - 2).start())
        guard(j >= 5, lambda: start(y_copies(j - 5)))

    def step(j, carry):
        bound(j, lambda c, f: pl.when(c)(f))
        total(j + 4, lax.max(j - 4, 0))
        mul(j)
        return carry

    m = n - 3
    lax.fori_loop(1, m, step, 0)

    bound(m, lambda c, f: f())
    total(m - 4)
    mul_oth(m)

    p_copy(m - 1).wait()
    pair_sum(m - 1)
    p_copy(m).start()
    a_copy(m - 3).wait()
    wait(y_copies(m - 5))
    a_copy(m - 1).start()
    start(y_copies(m - 4))
    total(m - 3)
    mul_own(m)

    p_copy(m).wait()
    pair_sum(m)
    start(y_copies(m - 3))
    wait(w_copies(m + 1))
    start(w_copies(m + 2))
    a_copy(m).start()
    mul_oth(m + 1)

    a_copy(m - 2).wait()
    wait(y_copies(m - 4))
    p_copy(m + 1).start()
    total(m - 2)
    mul_own(m + 1)

    p_copy(m + 1).wait()
    pair_sum(m + 1)
    a_copy(m - 1).wait()
    wait(y_copies(m - 3))
    start(y_copies(m - 2))
    wait(w_copies(m + 2))
    a_copy(m + 1).start()
    total(m - 1)
    mul_oth(m + 2)

    wait(y_copies(m - 2))
    p_copy(m + 2).start()
    start(y_copies(m - 1))
    mul_own(m + 2)

    p_copy(m + 2).wait()
    pair_sum(m + 2)
    wait(y_copies(m - 1))
    a_copy(m).wait()
    a_copy(m + 2).start()
    total(m)
    start(y_copies(m))
    a_copy(m + 1).wait()
    total(m + 1)
    wait(y_copies(m))
    start(y_copies(m + 1))
    a_copy(m + 2).wait()
    total(m + 2)
    start(y_copies(m + 2))
    wait(y_copies(m + 1))
    wait(y_copies(m + 2))


def solution(mesh):
    def per_device(x_one, x_two, w_down):
        mb, depth = x_one.shape
        width = w_down.shape[1]
        hbm = pl.BlockSpec(memory_space=pltpu.HBM)
        dma = pltpu.SemaphoreType.DMA
        return pl.pallas_call(
            kernel,
            out_shape=[pltpu.VMEM((mb, width), BF16)] * 2,
            in_specs=[hbm] * 3,
            out_specs=[pl.BlockSpec(memory_space=pltpu.VMEM)] * 2,
            scratch_shapes=[
                pltpu.VMEM((2 * mb, depth), BF16),
                pltpu.VMEM((2, depth, COLS), BF16),
                pltpu.VMEM((2, mb, COLS), F32),
                pltpu.VMEM((2, mb, COLS), F32),
                pltpu.VMEM((2, mb, COLS), F32),
                pltpu.VMEM((4, mb, COLS), BF16),
                pltpu.VMEM((8, mb, COLS), BF16),
                dma((PIECES, 4)), dma((PIECES,)), dma((2, 2)),
                dma((2,)), dma((2,)), dma((4,)), dma((8,)),
                dma((2, 2)), dma((4, 2)),
            ],
            compiler_params=pltpu.CompilerParams(
                collective_id=0, has_side_effects=True, vmem_limit_bytes=50 * 1024 * 1024),
        )(x_one, x_two, w_down)

    return jax.shard_map(
        per_device,
        mesh=mesh,
        in_specs=(P("data", "tp"), P("data", "tp"), P("tp", None)),
        out_specs=(P("data", None), P("data", None)),
        check_vma=False,
    )
```

```python
import jax
import jax.numpy as jnp
from jax import lax
from jax.experimental import pallas as pl
from jax.experimental.pallas import tpu as pltpu
from jax.sharding import PartitionSpec as P

MESH = pl.DeviceIdType.MESH
BF16 = jnp.bfloat16
F32 = jnp.float32

COLS = 512
PIECES = 6


def mod(j, n):
    return j % n if isinstance(j, int) else lax.rem(j, n)


def kernel(x1, x2, w, y1, y2, X, W, Ps, R, own, A, B,
           xsem, w0sem, wsem, p_send, p_recv, a_send, a_recv, y_send, y_recv):
    mb, depth = x1.shape
    width = w.shape[1]
    half = mb // 2
    n = width // COLS
    kp = depth // PIECES

    me = lax.axis_index("tp")
    core = lax.rem(me, 2)
    sib = me + 1 - 2 * core
    peer = lax.rem(me + 2, 4)
    r_own = pl.multiple_of(core * half, half)
    r_oth = pl.multiple_of((1 - core) * half, half)

    def col(j):
        return pl.ds(j * COLS if isinstance(j, int) else pl.multiple_of(j * COLS, COLS), COLS)

    def x_copies(i):
        ks = pl.ds(i * kp if isinstance(i, int) else pl.multiple_of(i * kp, kp), kp)
        return [
            pltpu.make_async_copy(src.at[pl.ds(row, half), ks], X.at[pl.ds(g * half, half), ks], xsem.at[i, g])
            for g, (src, row) in enumerate(((x1, r_oth), (x2, r_oth), (x1, r_own), (x2, r_own)))
        ]

    def w0_copy(i):
        ks = pl.ds(i * kp if isinstance(i, int) else pl.multiple_of(i * kp, kp), kp)
        return pltpu.make_async_copy(w.at[ks, col(0)], W.at[0, ks], w0sem.at[i])

    def w_copies(j):
        s = mod(j, 2)
        kh = depth // 2
        return [
            pltpu.make_async_copy(w.at[pl.ds(i * kh, kh), col(j)], W.at[s, pl.ds(i * kh, kh)], wsem.at[s, i])
            for i in range(2)
        ]

    def p_copy(j):
        s = mod(j, 2)
        return pltpu.make_async_remote_copy(
            src_ref=Ps.at[s], dst_ref=R.at[s], send_sem=p_send.at[s], recv_sem=p_recv.at[s],
            device_id={"tp": sib}, device_id_type=MESH)

    def a_copy(j):
        s, t = mod(j, 4), mod(j, 8)
        return pltpu.make_async_remote_copy(
            src_ref=A.at[s], dst_ref=B.at[t], send_sem=a_send.at[s], recv_sem=a_recv.at[t],
            device_id={"tp": peer}, device_id_type=MESH)

    def y_copies(j):
        s, t = mod(j, 2), mod(j, 4)
        out = []
        for g, y in enumerate((y1, y2)):
            ref = y.at[pl.ds(r_own, half), col(j)]
            out.append(pltpu.make_async_remote_copy(
                src_ref=ref, dst_ref=ref, send_sem=y_send.at[s, g], recv_sem=y_recv.at[t, g],
                device_id={"tp": sib}, device_id_type=MESH))
        return out

    def start(copies):
        for c in copies:
            c.start()

    def wait(copies):
        for c in copies:
            c.wait()

    def pair_sum(j):
        A[mod(j, 4)] = (own[mod(j, 2)] + R[mod(j, 2)]).astype(BF16)

    def total(j, c=None):
        v = (A[mod(j, 4)].astype(F32) + B[mod(j, 8)].astype(F32)).astype(BF16)
        for g, y in enumerate((y1, y2)):
            y[pl.ds(r_own, half), col(j if c is None else c)] = v[g * half : (g + 1) * half]

    def mul(j):
        s = mod(j, 2)
        d = jnp.dot(X[...], W[s], preferred_element_type=F32)
        Ps[s] = d[:mb]
        own[s] = d[mb:]

    def mul_oth(j):
        Ps[j % 2] = jnp.dot(X[pl.ds(0, mb), :], W[j % 2], preferred_element_type=F32)

    def mul_own(j):
        own[j % 2] = jnp.dot(X[pl.ds(mb, mb), :], W[j % 2], preferred_element_type=F32)

    for i in range(PIECES):
        start(x_copies(i))
        w0_copy(i).start()
    start(w_copies(1))

    barrier = pltpu.get_barrier_semaphore()
    for other in (sib, peer):
        pl.semaphore_signal(barrier, inc=1, device_id={"tp": other}, device_id_type=MESH)
    pl.semaphore_wait(barrier, 2)

    Ps[0] = jnp.zeros((mb, COLS), F32)
    own[0] = jnp.zeros((mb, COLS), F32)

    def first(i, carry):
        w0_copy(i).wait()
        wait(x_copies(i))
        ks = pl.ds(pl.multiple_of(i * kp, kp), kp)
        d = jnp.dot(X[:, ks], W[0, ks, :], preferred_element_type=F32)
        Ps[0] += d[:mb]
        own[0] += d[mb:]
        return carry

    lax.fori_loop(0, PIECES, first, 0)

    def bound(j, guard):
        wait(w_copies(j))

        guard(j >= 2, lambda: p_copy(j - 2).wait())
        pair_sum(j - 2 if isinstance(j, int) else j + 2)
        p_copy(j - 1).start()
        start(w_copies(j + 1))
        guard(j >= 4, lambda: a_copy(j - 4).wait())
        guard(j >= 6, lambda: wait(y_copies(j - 6)))
        guard(j >= 2, lambda: a_copy(j - 2).start())
        guard(j >= 5, lambda: start(y_copies(j - 5)))

    def step(j, carry):
        bound(j, lambda c, f: pl.when(c)(f))
        total(j + 4, lax.max(j - 4, 0))
        mul(j)
        return carry

    m = n - 3
    lax.fori_loop(1, m, step, 0)

    bound(m, lambda c, f: f())
    mul_oth(m)
    total(m - 4)

    p_copy(m - 1).wait()
    pair_sum(m - 1)
    p_copy(m).start()
    a_copy(m - 3).wait()
    wait(y_copies(m - 5))
    a_copy(m - 1).start()
    start(y_copies(m - 4))
    mul_own(m)
    total(m - 3)

    p_copy(m).wait()
    pair_sum(m)
    start(y_copies(m - 3))
    wait(w_copies(m + 1))
    start(w_copies(m + 2))
    a_copy(m).start()
    mul_oth(m + 1)

    a_copy(m - 2).wait()
    wait(y_copies(m - 4))
    p_copy(m + 1).start()
    mul_own(m + 1)
    total(m - 2)

    p_copy(m + 1).wait()
    pair_sum(m + 1)
    a_copy(m - 1).wait()
    wait(y_copies(m - 3))
    start(y_copies(m - 2))
    wait(w_copies(m + 2))
    a_copy(m + 1).start()
    mul_oth(m + 2)
    total(m - 1)

    wait(y_copies(m - 2))
    p_copy(m + 2).start()
    start(y_copies(m - 1))
    mul_own(m + 2)

    p_copy(m + 2).wait()
    pair_sum(m + 2)
    wait(y_copies(m - 1))
    a_copy(m).wait()
    a_copy(m + 2).start()
    total(m)
    start(y_copies(m))
    a_copy(m + 1).wait()
    total(m + 1)
    wait(y_copies(m))
    start(y_copies(m + 1))
    a_copy(m + 2).wait()
    total(m + 2)
    start(y_copies(m + 2))
    wait(y_copies(m + 1))
    wait(y_copies(m + 2))


def put_kernel(v1, v2, y1, y2, sem):
    rows, width = v1.shape
    part = width // 4
    copies = [
        pltpu.make_async_copy(v.at[:, pl.ds(i * part, part)], y.at[:, pl.ds(i * part, part)], sem.at[g, i])
        for g, (v, y) in enumerate(((v1, y1), (v2, y2)))
        for i in range(4)
    ]
    for c in copies:
        c.start()
    for c in copies:
        c.wait()


def solution(mesh):
    def per_device(x_one, x_two, w_down):
        mb, depth = x_one.shape
        width = w_down.shape[1]
        hbm = pl.BlockSpec(memory_space=pltpu.HBM)
        dma = pltpu.SemaphoreType.DMA
        totals = pl.pallas_call(
            kernel,
            out_shape=[pltpu.VMEM((mb, width), BF16)] * 2,
            in_specs=[hbm] * 3,
            out_specs=[pl.BlockSpec(memory_space=pltpu.VMEM)] * 2,
            scratch_shapes=[
                pltpu.VMEM((2 * mb, depth), BF16),
                pltpu.VMEM((2, depth, COLS), BF16),
                pltpu.VMEM((2, mb, COLS), F32),
                pltpu.VMEM((2, mb, COLS), F32),
                pltpu.VMEM((2, mb, COLS), F32),
                pltpu.VMEM((4, mb, COLS), BF16),
                pltpu.VMEM((8, mb, COLS), BF16),
                dma((PIECES, 4)), dma((PIECES,)), dma((2, 2)),
                dma((2,)), dma((2,)), dma((4,)), dma((8,)),
                dma((2, 2)), dma((4, 2)),
            ],
            compiler_params=pltpu.CompilerParams(
                collective_id=0, has_side_effects=True, vmem_limit_bytes=50 * 1024 * 1024),
        )(x_one, x_two, w_down)
        return pl.pallas_call(
            put_kernel,
            out_shape=[jax.ShapeDtypeStruct((mb, width), BF16)] * 2,
            in_specs=[pl.BlockSpec(memory_space=pltpu.VMEM)] * 2,
            out_specs=[hbm] * 2,
            scratch_shapes=[dma((2, 4))],
            compiler_params=pltpu.CompilerParams(vmem_limit_bytes=1024 * 1024),
        )(*totals)

    return jax.shard_map(
        per_device,
        mesh=mesh,
        in_specs=(P("data", "tp"), P("data", "tp"), P("tp", None)),
        out_specs=(P("data", None), P("data", None)),
        check_vma=False,
    )
```
